32 devices in a mesh: section: 2 (over core), seq: 4 (over y, x), head: 4 (over z).
Axes of the slice: x: 2, y: 2, z: 4, core: 2. Of those that a mesh axis runs over, the one named last changes fastest.
Arguments:
- x_in: bfloat16 [2, 1024, 8192], P('section', 'seq', 'head'), may hold values from -6 to 6
- b_in: bfloat16 [2, 1024, 2048], P('section', 'seq', 'head'), may hold values from -6 to 6
- c_in: bfloat16 [2, 1024, 2048], P('section', 'seq', 'head'), may hold values from -6 to 6
- z_in: bfloat16 [2, 1024, 8192], P('section', 'seq', 'head'), may hold values from -6 to 6
- dt_raw: float32 [2, 128, 1024], P('section', 'head', 'seq'), may hold values from -5 to 5
- conv_x: float32 [2, 4, 8192], P('section', None, 'head'), may hold values from -3 to 3
- conv_b: float32 [2, 4, 2048], P('section', None, 'head'), may hold values from -3 to 3
- conv_c: float32 [2, 4, 2048], P('section', None, 'head'), may hold values from -3 to 3
- a_rate: float32 [2, 128], P('section', 'head'), may hold values from 0.0001 to 1
- dt_bias: float32 [2, 128], P('section', 'head'), may hold values from -3 to -0.5
- skip_d: float32 [2, 128], P('section', 'head'), may hold values from 0.5 to 2
- norm_gain: float32 [2, 8192], P('section', 'head'), may hold values from 0.25 to 1.75
- out_weight: bfloat16 [2, 8192, 8192], P('section', 'head', 'seq'), may hold values from -0.0625 to 0.0625
Outputs:
- mixed: bfloat16 [2, 1024, 8192], P('section', ('seq', 'head'))
The draws below stay inside these ranges and needn't reach their ends.
All inputs are finite; a program needn't handle non-finite values.
Results may differ from the reference program's by a relative error of at most 0.007.
Values may be sent and summed in bfloat16 or wider, within the bound.
A program may use at most 128 MiB of HBM per device.

```python
import math
import jax
import jax.numpy as jnp
from jax import lax

D = 8192
P_SIZE = 64
N = 256
G = 8
KCONV = 4
HEADS = 128
TOK_DEV = 256
INNER = 8192
TOKENS = 1024
SECTIONS = 2


def draw_a_rate(key, part):
    lowest = math.log(0.0002)
    highest = math.log(1.0)
    exponent = jax.random.uniform(key, (SECTIONS, HEADS), jnp.float32, lowest, highest)
    return jnp.exp(exponent)


def level_of(key, shape, shards, low, top_value):
    level, own = 1.0, jax.random.fold_in(key, 6)
    for position, blocks in shards:
        draws = jnp.exp(jax.random.uniform(jax.random.fold_in(own, position), (blocks,), jnp.float32, low / len(shards), top_value / len(shards)))
        level = level * jnp.repeat(draws, shape[position] // blocks).reshape([-1 if axis == position else 1 for axis in range(len(shape))])
    return level


def gaussian(key, extent, width, bound, pieces=(), kind=jnp.bfloat16):
    gain = level_of(key, extent, pieces, -0.22, 0.18) if pieces else 1.0
    entries = jax.random.normal(key, extent, jnp.float32) * width * gain
    return jnp.minimum(jnp.maximum(entries, -bound), bound).astype(kind)


def setup_inputs(seed: int = 0) -> dict:
    key_of = jax.random.split(jax.random.key(seed), 14)
    return {
        "x_in": gaussian(key_of[0], (SECTIONS, TOKENS, INNER), 1.0, 6.0, ((0, 2), (1, 4), (2, 4))),
        "b_in": gaussian(key_of[1], (SECTIONS, TOKENS, G * N), 1.0, 6.0, ((0, 2), (1, 4), (2, 4))),
        "c_in": gaussian(key_of[2], (SECTIONS, TOKENS, G * N), 1.0, 6.0, ((0, 2), (1, 4), (2, 4))),
        "z_in": gaussian(key_of[3], (SECTIONS, TOKENS, INNER), 1.0, 6.0, ((0, 2), (1, 4), (2, 4))),
        "dt_raw": gaussian(key_of[4], (SECTIONS, HEADS, TOKENS), 1.0, 5.0, ((0, 2), (1, 4), (2, 4)), jnp.float32),
        "conv_x": gaussian(key_of[5], (SECTIONS, KCONV, INNER), KCONV ** -0.5, 3.0, ((0, 2), (2, 4)), jnp.float32),
        "conv_b": gaussian(key_of[6], (SECTIONS, KCONV, G * N), KCONV ** -0.5, 3.0, ((0, 2), (2, 4)), jnp.float32),
        "conv_c": gaussian(key_of[7], (SECTIONS, KCONV, G * N), KCONV ** -0.5, 3.0, ((0, 2), (2, 4)), jnp.float32),
        "a_rate": draw_a_rate(jax.random.fold_in(key_of[13], 71), 0),
        "dt_bias": jnp.clip(-3.0 + 2.5 * jax.random.uniform(key_of[9], (SECTIONS, HEADS), jnp.float32) ** level_of(key_of[9], (SECTIONS, HEADS), ((0, 2), (1, 4)), -0.2, 0.2), -3.0, -0.5),
        "skip_d": jnp.clip(0.5 + 1.5 * jax.random.uniform(key_of[10], (SECTIONS, HEADS), jnp.float32) ** level_of(key_of[10], (SECTIONS, HEADS), ((0, 2), (1, 4)), -0.2, 0.2), 0.5, 2.0),
        "norm_gain": jnp.clip(1.0 + 0.15 * jax.random.normal(key_of[11], (SECTIONS, INNER), jnp.float32), 0.25, 1.75),
        "out_weight": gaussian(key_of[12], (SECTIONS, INNER, D), INNER ** -0.5, 0.0625, ((0, 2), (1, 4), (2, 4))),
    }


epsilon = 1e-05

def conv_silu(signal, kernel):
    kernel_taps = kernel.shape[0]
    length = signal.shape[0]
    padded = jnp.pad(signal, ((kernel_taps - 1, 0), (0, 0)))
    summed = jnp.zeros(signal.shape, jnp.float32)
    for offset in range(kernel_taps):
        summed = summed + kernel[offset] * padded[offset:offset + length].astype(jnp.float32)
    return jax.nn.silu(summed).astype(jnp.bfloat16)

def one_layer(x_in, b_in, c_in, z_in, dt_raw, conv_x, conv_b, conv_c, a_rate, dt_bias, skip_d, norm_gain, out_weight):
    x_conv = conv_silu(x_in, conv_x)
    b_conv = conv_silu(b_in, conv_b)
    c_conv = conv_silu(c_in, conv_c)
    step_size = jax.nn.softplus(dt_raw + dt_bias[:, None])
    step_log = -a_rate[:, None] * step_size
    blocks = TOKENS // TOK_DEV
    per_group = HEADS // G
    x_blocks = x_conv.reshape(blocks, TOK_DEV, G, per_group, P_SIZE)
    b_blocks = b_conv.reshape(blocks, TOK_DEV, G, N)
    c_blocks = c_conv.reshape(blocks, TOK_DEV, G, N)
    z_blocks = z_in.reshape(blocks, TOK_DEV, INNER)
    step_blocks = jnp.transpose(step_size.reshape(G, per_group, blocks, TOK_DEV), (2, 0, 1, 3))
    log_blocks = jnp.transpose(step_log.reshape(G, per_group, blocks, TOK_DEV), (2, 0, 1, 3))
    causal = jnp.arange(TOK_DEV)[:, None] >= jnp.arange(TOK_DEV)[None, :]
    skip_term = skip_d.reshape(G, per_group)

    def block_step(carried, inputs):
        x_block, b_block, c_block, z_block, step_block, log_block = inputs
        log_decay = jnp.cumsum(log_block, axis=2)
        scores = jnp.einsum('tgn,ugn->gtu', c_block.astype(jnp.float32), b_block.astype(jnp.float32))
        spread_log = log_decay[:, :, :, None] - log_decay[:, :, None, :]
        damping = jnp.where(causal, jnp.exp(jnp.minimum(spread_log, 0.0)), 0.0)
        weights = (damping * step_block[:, :, None, :] * scores[:, None]).astype(jnp.bfloat16)
        weights = lax.optimization_barrier(weights).astype(jnp.float32)
        inside = jnp.einsum('gjtu,ugjp->tgjp', weights, x_block.astype(jnp.float32))
        to_end = jnp.exp(log_decay[:, :, -1:] - log_decay) * step_block
        x_weighted = (x_block.astype(jnp.float32) * jnp.transpose(to_end, (2, 0, 1))[..., None]).astype(jnp.bfloat16)
        x_weighted = lax.optimization_barrier(x_weighted).astype(jnp.float32)
        block_sum = jnp.einsum('ugjp,ugn->gjpn', x_weighted, b_block.astype(jnp.float32))
        block_decay = jnp.exp(log_decay[:, :, -1])
        carried_b = lax.optimization_barrier(carried.astype(jnp.bfloat16)).astype(jnp.float32)
        outside = jnp.einsum('tgn,gjpn->tgjp', c_block.astype(jnp.float32), carried_b)
        outside = outside * jnp.transpose(jnp.exp(log_decay), (2, 0, 1))[..., None]
        out_ssm = inside + outside + skip_term[None, :, :, None] * x_block.astype(jnp.float32)
        gated = out_ssm.reshape(TOK_DEV, G, per_group * P_SIZE) * jax.nn.silu(z_block.astype(jnp.float32)).reshape(TOK_DEV, G, per_group * P_SIZE)
        inverse_rms = lax.rsqrt(lax.optimization_barrier(jnp.mean(gated * gated, axis=2, keepdims=True)) + epsilon)
        hidden = ((gated * inverse_rms).reshape(TOK_DEV, INNER) * norm_gain).astype(jnp.bfloat16)
        new_carried = block_decay[:, :, None, None] * carried + block_sum
        return (new_carried, hidden)
    start = jnp.zeros((G, per_group, P_SIZE, N), jnp.float32)
    final_state, hidden = lax.scan(block_step, start, (x_blocks, b_blocks, c_blocks, z_blocks, step_blocks, log_blocks))
    hidden = hidden.reshape(TOKENS, INNER)
    return jnp.dot(hidden, out_weight, preferred_element_type=jnp.float32).astype(jnp.bfloat16)

def reference(x_in, b_in, c_in, z_in, dt_raw, conv_x, conv_b, conv_c, a_rate, dt_bias, skip_d, norm_gain, out_weight):
    layers = []
    for section_index in range(SECTIONS):
        layers.append(one_layer(x_in[section_index], b_in[section_index], c_in[section_index], z_in[section_index], dt_raw[section_index], conv_x[section_index], conv_b[section_index], conv_c[section_index], a_rate[section_index], dt_bias[section_index], skip_d[section_index], norm_gain[section_index], out_weight[section_index]))
    stacked = jnp.stack(layers)
    return jnp.roll(stacked, 1, axis=0)
```

```python
import functools

import jax
import jax.numpy as jnp
from jax import lax
from jax.experimental import pallas as pl
from jax.experimental.pallas import tpu as pltpu
from jax.sharding import PartitionSpec as P

N = 256


epsilon = 1e-05


def partner(place, bits):
    bit = 1
    while bit <= bits:
        if bits & bit:
            place = place + bit - 2 * bit * ((place // bit) % 2)
        bit *= 2
    return place


def project_kernel(
    sizes, hid, weight, out, w_buf, got, part, landed, summed,
    w_sem, ag_send, ag_recv, z_send, z_recv, o_send, o_recv,
):
    sections, shards, heads = sizes
    halves, count, _ = hid.shape
    rows, width = part.shape[3], part.shape[4]
    tile = min(512, width)
    here_s, here_h = lax.axis_index("seq"), lax.axis_index("head")
    other = lax.rem(lax.axis_index("section") + 1, sections)
    load = pltpu.make_async_copy(weight, w_buf, w_sem)
    load.start()
    barrier = pltpu.get_barrier_semaphore()
    for d in range(shards):
        if d:
            pl.semaphore_signal(barrier, inc=1, device_id={"seq": partner(here_s, d)})
        pl.semaphore_signal(
            barrier, inc=1, device_id={"section": other, "seq": partner(here_s, d)}
        )
    for e in range(1, heads):
        pl.semaphore_signal(barrier, inc=1, device_id={"head": partner(here_h, e)})
    pl.semaphore_wait(barrier, 2 * shards - 1 + heads - 1)

    def gather(q, d):
        return pltpu.make_async_remote_copy(
            hid.at[q], got.at[q, d - 1], ag_send.at[q, d], ag_recv.at[q, d],
            device_id={"seq": partner(here_s, d)},
        )

    bits = [1 << k for k in range(heads.bit_length() - 1)]

    def exchange(q, d, bit):
        first = heads - heads // bit
        return [
            pltpu.make_async_remote_copy(
                part.at[q, d, partner(here_h, e + bit)], landed.at[q, d, first + n],
                z_send.at[q, d, first + n], z_recv.at[q, d, first + n],
                device_id={"head": partner(here_h, bit)},
            )
            for n, e in enumerate(range(0, heads, 2 * bit))
        ]

    def deliver(q, d):
        return pltpu.make_async_remote_copy(
            summed.at[q, d], out.at[q, here_s], o_send.at[q, d], o_recv.at[q, d],
            device_id={"section": other, "seq": partner(here_s, d)},
        )

    for q in range(halves):
        for d in range(1, shards):
            gather(q, d).start()
    load.wait()

    def multiply(q, d):
        rows_in = hid.at[q] if d == 0 else got.at[q, d - 1]

        def one(i, _):
            cols = pl.ds(pl.multiple_of(i * tile, tile), tile)
            terms = jnp.dot(rows_in[...], w_buf[:, cols], preferred_element_type=jnp.float32)
            part[q, d, :, :, cols] = terms.astype(jnp.bfloat16).reshape(heads, rows, tile)
            return 0

        lax.fori_loop(0, width // tile, one, 0)

    def advance(q, d, k):
        bit = bits[k]
        first = heads - heads // bit
        for n, copy in enumerate(exchange(q, d, bit)):
            copy.wait_recv()
            mine = partner(here_h, 2 * bit * n)
            total = part[q, d, mine].astype(jnp.float32)
            total = (total + landed[q, d, first + n].astype(jnp.float32)).astype(jnp.bfloat16)
            if k + 1 < len(bits):
                part[q, d, mine] = total
            else:
                summed[q, d] = total
        if k + 1 < len(bits):
            for copy in exchange(q, d, bits[k + 1]):
                copy.start()
        else:
            deliver(q, d).start()

    units = [(q, 0) for q in range(halves)]
    units += [(q, d) for q in range(halves) for d in range(1, shards)]
    for n in range(len(units) + len(bits)):
        if n < len(units):
            q, d = units[n]
            if d:
                gather(q, d).wait_recv()
            multiply(q, d)
            for copy in exchange(q, d, bits[0]):
                copy.start()
        for k in range(len(bits)):
            if 0 <= n - 1 - k < len(units):
                advance(*units[n - 1 - k], k)
    for q, d in units:
        if d:
            gather(q, d).wait_send()
        for bit in bits:
            for copy in exchange(q, d, bit):
                copy.wait_send()
        deliver(q, d).wait_send()
        pltpu.make_async_remote_copy(
            summed.at[q, d], out.at[q, partner(here_s, d)], o_send.at[q, d], o_recv.at[q, d],
            device_id={"section": other, "seq": partner(here_s, d)},
        ).wait_recv()


def project(hid, weight, sizes):
    sections, shards, heads = sizes
    halves, count, depth = hid.shape
    width = weight.shape[1]
    rows = count // heads
    bf16 = jnp.bfloat16
    dma = pltpu.SemaphoreType.DMA
    flops = 2 * halves * count * shards * depth * width
    return pl.pallas_call(
        functools.partial(project_kernel, sizes),
        out_shape=jax.ShapeDtypeStruct((halves, shards, rows, width), bf16),
        in_specs=[pl.BlockSpec(memory_space=pltpu.VMEM), pl.BlockSpec(memory_space=pl.ANY)],
        out_specs=pl.BlockSpec(memory_space=pl.ANY),
        scratch_shapes=[
            pltpu.VMEM(weight.shape, bf16),
            pltpu.VMEM((halves, shards - 1, count, depth), bf16),
            pltpu.VMEM((halves, shards, heads, rows, width), bf16),
            pltpu.VMEM((halves, shards, heads - 1, rows, width), bf16),
            pltpu.VMEM((halves, shards, rows, width), bf16),
            dma,
            dma((halves, shards)),
            dma((halves, shards)),
            dma((halves, shards, heads)),
            dma((halves, shards, heads)),
            dma((halves, shards)),
            dma((halves, shards)),
        ],
        compiler_params=pltpu.CompilerParams(
            collective_id=0, has_side_effects=True, vmem_limit_bytes=48 * 2**20
        ),
        cost_estimate=pl.CostEstimate(
            flops=flops, bytes_accessed=2 * weight.size, transcendentals=0
        ),
        name="project",
    )(hid, weight)


def mix_kernel(
    shards, dims, x_hbm, b_hbm, c_hbm, z_hbm, dt_hbm, kx_hbm, kb_hbm, kc_hbm, a_hbm, bias_hbm,
    skip_hbm, gain_hbm, hid, x, b, c, z, dt, kx, kb, kc, a, bias, skip, gain, loaded,
    ex, eb, ec, pad, xc, bt, cc, sc, vec, dtp, ldrow, steprow, ldcol, cat, tocat,
    eld, sums, acc, ssq, inbox, outbox, e_send, e_recv, send, recv,
):
    head_dim, chunk, heads_z, halves = dims
    f32, bf16 = jnp.float32, jnp.bfloat16
    me = lax.axis_index("seq")
    length, width = x.shape
    head_count = dt.shape[0]
    groups = sc.shape[0]
    state = bt.shape[1]
    taps = kx.shape[0]
    edge = ex.shape[0]
    chunks = width // chunk
    per_chunk = chunk // head_dim
    group_chunks = chunks // groups
    lanes = 128
    after, before = lax.rem(me + 1, shards), lax.rem(me + shards - 1, shards)
    first, last = me == 0, me == shards - 1
    froms = (b_hbm, c_hbm, x_hbm, dt_hbm, kx_hbm, kb_hbm, kc_hbm, a_hbm, bias_hbm, skip_hbm)
    tos = (b, c, x, dt, kx, kb, kc, a, bias, skip)
    froms, tos = froms + (z_hbm, gain_hbm), tos + (z, gain)
    loads = [
        pltpu.make_async_copy(src, dst, loaded.at[n])
        for n, (src, dst) in enumerate(zip(froms, tos))
    ]
    for load in loads:
        load.start()
    barrier = pltpu.get_barrier_semaphore()
    for neighbour in (before, after):
        pl.semaphore_signal(barrier, inc=1, device_id={"seq": neighbour})
    pl.semaphore_wait(barrier, 2)

    edges = [
        pltpu.make_async_remote_copy(
            src.at[pl.ds(length - edge, edge)], dst, e_send.at[n], e_recv.at[n],
            device_id={"seq": after},
        )
        for n, (src, dst) in enumerate(((x_hbm, ex), (b_hbm, eb), (c_hbm, ec)))
    ]

    def hand_on(k):
        return pltpu.make_async_remote_copy(
            outbox.at[k], inbox.at[k], send.at[k], recv.at[k], device_id={"seq": after}
        )

    @pl.when(jnp.logical_not(last))
    def _():
        for copy in edges:
            copy.start()

    @pl.when(first)
    def _():
        for dst in (ex, eb, ec):
            dst[...] = jnp.zeros(dst.shape, dst.dtype)

    for load in loads:
        load.wait()

    vec[...] = jnp.zeros(vec.shape, f32)
    dtp[...] = jnp.zeros(dtp.shape, f32)
    dtp[:head_count, :] = dt[...]
    for n, ref in enumerate((a, bias, skip)):
        vec[8 * n : 8 * n + 1, :head_count] = ref[...]
    step = jax.nn.softplus(dtp[...].T + vec[8:9, :])
    rows = lax.broadcasted_iota(jnp.int32, (length, length), 0)
    columns = lax.broadcasted_iota(jnp.int32, (length, length), 1)
    causal = rows >= columns
    decay = jnp.dot(
        jnp.where(causal, 1.0, 0.0), -vec[0:1, :] * step,
        precision=lax.Precision.HIGHEST, preferred_element_type=f32,
    )
    ldrow[...] = decay.T
    steprow[...] = step.T
    for k in range(chunks):
        ldcol[k] = decay[:, k * per_chunk : (k + 1) * per_chunk]

    def split(dst, value, first_row):
        size = value.shape[0]
        for n in range(3):
            part = value.astype(bf16)
            dst[n, first_row : first_row + size, :] = part
            value = value - part.astype(f32)

    split(cat, jnp.exp(decay), 0)
    split(cat, jnp.broadcast_to(vec[16:17, :], (16, lanes)), length)
    split(tocat, jnp.exp(decay[length - 1 : length, :] - decay) * step, 0)

    def conv(src, border, kernel, cols):
        pad[0:edge, :] = border[:, cols].astype(f32)
        pad[edge:, :] = src[:, cols].astype(f32)
        total = jnp.zeros((length, pad.shape[1]), f32)
        for k in range(taps):
            start = edge - taps + 1 + k
            total = total + kernel[k : k + 1, cols] * pad[start : start + length, :]
        return total * jax.nn.sigmoid(total)

    @pl.when(me > 0)
    def _():
        for copy in edges:
            copy.wait_recv()

    for g in range(groups):
        cols = slice(g * state, (g + 1) * state)
        b_conv = conv(b, eb, kb, cols).astype(bf16)
        bt[g] = b_conv.astype(f32).T.astype(bf16)
        cc[:, cols] = conv(c, ec, kc, cols).astype(bf16)
        scores = jnp.dot(cc[:, cols], bt[g], preferred_element_type=f32)
        sc[g] = jnp.where(causal, scores, 0.0)

    def spread(src, k):
        head = lax.broadcasted_iota(jnp.int32, (lanes, chunk), 0) - k * per_chunk
        lane = lax.broadcasted_iota(jnp.int32, (lanes, chunk), 1)
        start = head * head_dim
        pick = jnp.where((lane >= start) & (lane < start + head_dim), 1.0, 0.0).astype(bf16)
        total = jnp.dot(src[0], pick, preferred_element_type=f32)
        for n in range(1, 3):
            total = total + jnp.dot(src[n], pick, preferred_element_type=f32)
        return total

    def gather_state(k, _):
        cols = pl.ds(pl.multiple_of(k * chunk, chunk), chunk)
        x_conv = conv(x, ex, kx, cols).astype(bf16)
        xc[:, cols] = x_conv
        eld[:, cols] = spread(cat, k)
        weighted = (x_conv.astype(f32) * spread(tocat, k)).astype(bf16)
        total = jnp.dot(bt[k // group_chunks], weighted, preferred_element_type=f32)
        sums[:, cols] = total

        @pl.when(first)
        def _():
            outbox[k] = total.astype(bf16)
            hand_on(k).start()

        return 0

    lax.fori_loop(0, chunks, gather_state, 0)
    per_tile = lanes // head_dim

    def finish(k, _):
        cols = pl.ds(pl.multiple_of(k * chunk, chunk), chunk)
        g = k // group_chunks
        scores = sc[g]
        columns_of = ldcol[k]
        for j in range(chunk // lanes):
            tile = pl.ds(pl.multiple_of(k * chunk + j * lanes, lanes), lanes)
            x_tile = xc[:, tile]
            lane = lax.broadcasted_iota(jnp.int32, (length, lanes), 1)
            inside = None
            for i in range(per_tile):
                n = j * per_tile + i
                h = k * per_chunk + n
                gap = columns_of[:, n : n + 1] - ldrow[pl.ds(h, 1), :]
                damping = jnp.exp(jnp.minimum(gap, 0.0))
                weights = (damping * steprow[pl.ds(h, 1), :] * scores).astype(bf16)
                term = jnp.dot(weights, x_tile, preferred_element_type=f32)
                inside = term if i == 0 else jnp.where(lane >= i * head_dim, term, inside)
            acc[:, tile] = inside

        @pl.when(me > 0)
        def _():
            hand_on(k).wait_recv()

            @pl.when(jnp.logical_not(last))
            def _():
                old = eld[length - 1 : length, cols] * inbox[k].astype(f32)
                outbox[k] = (old + sums[:, cols]).astype(bf16)
                hand_on(k).start()

            c_group = cc[:, pl.ds(pl.multiple_of(g * state, state), state)]
            outside = jnp.dot(c_group, inbox[k], preferred_element_type=f32)
            acc[:, cols] = acc[:, cols] + outside * eld[:length, cols]

        z_here = z[:, cols].astype(f32)
        total = acc[:, cols] + eld[length : length + 1, cols] * xc[:, cols].astype(f32)
        gated = total * (z_here * jax.nn.sigmoid(z_here))
        acc[:, cols] = gated
        square = gated * gated
        part = square[:, :lanes]
        for j in range(1, chunk // lanes):
            part = part + square[:, j * lanes : (j + 1) * lanes]
        ssq[...] = jnp.where(lax.rem(k, group_chunks) == 0, part, ssq[...] + part)

        @pl.when(lax.rem(k, group_chunks) == group_chunks - 1)
        def _():
            mean = jnp.sum(ssq[...], axis=1, keepdims=True) / (group_chunks * chunk)
            scale = lax.rsqrt(mean + epsilon)
            count = length // (heads_z * halves)
            for j in range(group_chunks):
                first_col = (k - group_chunks + 1 + j) * chunk
                here = pl.ds(pl.multiple_of(first_col, chunk), chunk)
                value = (acc[:, here] * scale * gain[:, here]).astype(bf16)
                for e in range(heads_z):
                    for q in range(halves):
                        row = (e * halves + q) * count
                        hid[q, e * count : (e + 1) * count, here] = value[row : row + count]

        return 0

    lax.fori_loop(0, chunks, finish, 0)

    @pl.when(jnp.logical_not(last))
    def _():
        for copy in edges:
            copy.wait_send()

        def drain(k, _):
            hand_on(k).wait_send()
            return 0

        lax.fori_loop(0, chunks, drain, 0)


def mix(args, sizes, halves):
    x, b, c, z, dt, kx, kb, kc, a, bias, skip, gain = args
    sections, shards, heads_z = sizes
    length, width = x.shape
    head_count = dt.shape[0]
    head_dim = width // head_count
    groups = b.shape[1] // N
    chunk, lanes, edge = 256, 128, 8
    chunks = width // chunk
    f32, bf16 = jnp.float32, jnp.bfloat16
    dma = pltpu.SemaphoreType.DMA
    vmem = pltpu.VMEM
    count = length // halves
    return pl.pallas_call(
        functools.partial(mix_kernel, shards, (head_dim, chunk, heads_z, halves)),
        out_shape=jax.ShapeDtypeStruct((halves, count, width), bf16),
        in_specs=[pl.BlockSpec(memory_space=pl.ANY)] * 12,
        out_specs=pl.BlockSpec(memory_space=vmem),
        scratch_shapes=[vmem(array.shape, array.dtype) for array in args]
        + [
            dma((12,)),
            vmem((edge, width), bf16),
            vmem((edge, b.shape[1]), bf16),
            vmem((edge, b.shape[1]), bf16),
            vmem((edge + length, chunk), f32),
            vmem((length, width), bf16),
            vmem((groups, N, length), bf16),
            vmem((length, groups * N), bf16),
            vmem((groups, length, length), f32),
            vmem((24, lanes), f32),
            vmem((lanes, length), f32),
            vmem((lanes, length), f32),
            vmem((lanes, length), f32),
            vmem((chunks, length, chunk // head_dim), f32),
            vmem((3, length + 16, lanes), bf16),
            vmem((3, length, lanes), bf16),
            vmem((length + 16, width), f32),
            vmem((N, width), f32),
            vmem((length, width), f32),
            vmem((length, lanes), f32),
            vmem((chunks, N, chunk), bf16),
            vmem((chunks, N, chunk), bf16),
            dma((3,)),
            dma((3,)),
            dma((chunks,)),
            dma((chunks,)),
        ],
        compiler_params=pltpu.CompilerParams(
            collective_id=1, has_side_effects=True, vmem_limit_bytes=63 * 2**20
        ),
        cost_estimate=pl.CostEstimate(
            flops=2 * length * length * width * 4, bytes_accessed=8 * x.size, transcendentals=0
        ),
        name="mix",
    )(*args)


def per_device(
    x_in,
    b_in,
    c_in,
    z_in,
    dt_raw,
    conv_x,
    conv_b,
    conv_c,
    a_rate,
    dt_bias,
    skip_d,
    norm_gain,
    out_weight,
):
    sizes = tuple(lax.axis_size(name) for name in ("section", "seq", "head"))
    halves = 2
    whole = (x_in, b_in, c_in, z_in, dt_raw, conv_x, conv_b, conv_c)
    args = [array[0] for array in whole] + [a_rate, dt_bias, skip_d, norm_gain]
    hid = mix(args, sizes, halves)
    rows = x_in.shape[1] // (sizes[2] * halves)
    mixed = project(hid, out_weight[0], sizes)
    return jnp.transpose(mixed, (0, 2, 1, 3)).reshape(1, halves * rows, -1)


def solution(mesh):
    return jax.shard_map(
        per_device,
        mesh=mesh,
        in_specs=(
            P("section", "seq", "head"),
            P("section", "seq", "head"),
            P("section", "seq", "head"),
            P("section", "seq", "head"),
            P("section", "head", "seq"),
            P("section", None, "head"),
            P("section", None, "head"),
            P("section", None, "head"),
            P("section", "head"),
            P("section", "head"),
            P("section", "head"),
            P("section", "head"),
            P("section", "head", "seq"),
        ),
        out_specs=P("section", ("seq", "head"), None),
        check_vma=False,
    )
```

```python
import functools

import jax
import jax.numpy as jnp
from jax import lax
from jax.experimental import pallas as pl
from jax.experimental.pallas import tpu as pltpu
from jax.sharding import PartitionSpec as P

N = 256


epsilon = 1e-05


def partner(place, bits, size):
    bit = 1
    while bit < size:
        flip = (bits // bit) % 2
        place = place + flip * (bit - 2 * bit * ((place // bit) % 2))
        bit *= 2
    return place


def layer_kernel(
    sizes, dims, x_hbm, b_hbm, c_hbm, z_hbm, dt_hbm, kx_hbm, kb_hbm, kc_hbm, a_hbm, bias_hbm,
    skip_hbm, gain_hbm, weight, out, x, b, c, z, dt, kx, kb, kc, a, bias, skip, gain, loaded,
    ex, eb, ec, pad, xc, bt, cc, sc, vec, dtp, ldrow, steprow, ldcol, cat, tocat,
    eld, sums, acc, ssq, inbox, outbox, e_send, e_recv, send, recv,
    w_buf, got, part, up, down,
    w_sem, ag_send, ag_recv, u_send, u_recv, d_send, d_recv, o_send, o_recv,
):
    sections, shards, heads = sizes
    head_dim, chunk, halves, lag = dims
    count = got.shape[1]
    units = shards * halves
    rows, width = part.shape[2], part.shape[3]
    tile = min(512, width)
    tiles = width // tile
    f32, bf16 = jnp.float32, jnp.bfloat16
    here_s, h_z = lax.axis_index("seq"), lax.axis_index("head")
    end = heads - 1
    other = lax.rem(lax.axis_index("section") + 1, sections)
    me = here_s
    length, inner = x.shape
    head_count = dt.shape[0]
    groups = sc.shape[0]
    state = bt.shape[1]
    taps = kx.shape[0]
    edge = ex.shape[0]
    chunks = inner // chunk
    per_chunk = chunk // head_dim
    group_chunks = chunks // groups
    lanes = 128
    after, before = lax.rem(me + 1, shards), lax.rem(me + shards - 1, shards)
    first, last = me == 0, me == shards - 1
    froms = (dt_hbm, a_hbm, bias_hbm, skip_hbm, kb_hbm, kx_hbm, b_hbm, x_hbm)
    tos = (dt, a, bias, skip, kb, kx, b, x)
    small, early = 4, len(tos)
    froms, tos = froms + (kc_hbm, c_hbm, z_hbm, gain_hbm), tos + (kc, c, z, gain)
    loads = [
        pltpu.make_async_copy(src, dst, loaded.at[n])
        for n, (src, dst) in enumerate(zip(froms, tos))
    ]
    for load in loads:
        load.start()
    w_loads = [
        pltpu.make_async_copy(
            weight.at[:, pl.ds(i * tile, tile)], w_buf.at[:, pl.ds(i * tile, tile)], w_sem.at[i]
        )
        for i in range(tiles)
    ]
    barrier = pltpu.get_barrier_semaphore()
    for d in range(shards):
        peer = partner(here_s, d, shards)
        if d:
            pl.semaphore_signal(barrier, inc=1, device_id={"seq": peer})
        pl.semaphore_signal(barrier, inc=1, device_id={"section": other, "seq": peer})

    @pl.when(h_z > 0)
    def _():
        pl.semaphore_signal(barrier, inc=1, device_id={"head": h_z - 1})

    @pl.when(h_z < end)
    def _():
        pl.semaphore_signal(barrier, inc=1, device_id={"head": h_z + 1})

    near = jnp.where(h_z > 0, 1, 0) + jnp.where(h_z < end, 1, 0)
    pl.semaphore_wait(barrier, 2 * shards - 1 + near)

    edges = [
        pltpu.make_async_remote_copy(
            src.at[pl.ds(length - edge, edge)], dst, e_send.at[n], e_recv.at[n],
            device_id={"seq": after},
        )
        for n, (src, dst) in enumerate(((x_hbm, ex), (b_hbm, eb), (c_hbm, ec)))
    ]

    pieces = outbox.shape[1]
    piece = outbox.shape[3]

    def hand_on(k, i):
        return pltpu.make_async_remote_copy(
            outbox.at[k, i], inbox.at[k, i], send.at[k, i], recv.at[k, i],
            device_id={"seq": after},
        )

    @pl.when(jnp.logical_not(last))
    def _():
        for copy in edges:
            copy.start()

    @pl.when(first)
    def _():
        for dst in (ex, eb, ec):
            dst[...] = jnp.zeros(dst.shape, dst.dtype)

    for load in loads[:small]:
        load.wait()

    vec[...] = jnp.zeros(vec.shape, f32)
    dtp[...] = jnp.zeros(dtp.shape, f32)
    dtp[:head_count, :] = dt[...]
    for n, ref in enumerate((a, bias, skip)):
        vec[8 * n : 8 * n + 1, :head_count] = ref[...]
    step = jax.nn.softplus(dtp[...].T + vec[8:9, :])
    causal = lax.broadcasted_iota(jnp.int32, (length, length), 0) >= lax.broadcasted_iota(
        jnp.int32, (length, length), 1
    )
    below = jnp.where(causal, 1.0, 0.0).astype(bf16)
    rest = -vec[0:1, :] * step
    decay = jnp.zeros((length, lanes), f32)
    for _ in range(3):
        high = rest.astype(bf16)
        decay = decay + jnp.dot(below, high, preferred_element_type=f32)
        rest = rest - high.astype(f32)
    ldrow[...] = decay.T
    steprow[...] = step.T
    for k in range(chunks):
        ldcol[k] = decay[:, k * per_chunk : (k + 1) * per_chunk]

    def split(dst, value, first_row):
        size = value.shape[0]
        high = value.astype(bf16)
        dst[first_row : first_row + size, :lanes] = high
        dst[first_row : first_row + size, lanes:] = (value - high.astype(f32)).astype(bf16)

    split(cat, jnp.exp(decay), 0)
    split(cat, jnp.broadcast_to(vec[16:17, :], (16, lanes)), length)
    split(tocat, jnp.exp(decay[length - 1 : length, :] - decay) * step, 0)

    for load in loads[small:early]:
        load.wait()
    for load in w_loads:
        load.start()

    def conv(src, border, kernel, cols):
        pad[0:edge, :] = border[:, cols].astype(f32)
        pad[edge:, :] = src[:, cols].astype(f32)
        total = jnp.zeros((length, pad.shape[1]), f32)
        for k in range(taps):
            start = edge - taps + 1 + k
            total = total + kernel[k : k + 1, cols] * pad[start : start + length, :]
        return total * jax.nn.sigmoid(total)

    @pl.when(me > 0)
    def _():
        for copy in edges:
            copy.wait_recv()

    def ready(g):
        cols = pl.ds(pl.multiple_of(g * state, state), state)
        bt[g] = conv(b, eb, kb, cols).astype(bf16).astype(f32).T.astype(bf16)

    def spread(src, k):
        head = lax.broadcasted_iota(jnp.int32, (lanes, chunk), 0) - k * per_chunk
        lane = lax.broadcasted_iota(jnp.int32, (lanes, chunk), 1)
        start = head * head_dim
        pick = jnp.where((lane >= start) & (lane < start + head_dim), 1.0, 0.0).astype(bf16)
        pick = jnp.concatenate([pick, pick], axis=0)
        return jnp.dot(src[...], pick, preferred_element_type=f32)

    def gather_state(k, _):
        @pl.when(lax.rem(k, group_chunks) == 0)
        def _():
            ready(k // group_chunks)

        cols = pl.ds(pl.multiple_of(k * chunk, chunk), chunk)
        x_conv = conv(x, ex, kx, cols).astype(bf16)
        xc[:, cols] = x_conv
        eld[:, cols] = spread(cat, k)
        weighted = (x_conv.astype(f32) * spread(tocat, k)).astype(bf16)
        total = jnp.dot(bt[k // group_chunks], weighted, preferred_element_type=f32)
        sums[:, cols] = total

        @pl.when(first)
        def _():
            for i in range(pieces):
                outbox[k, i] = total[:, i * piece : (i + 1) * piece].astype(bf16)
                hand_on(k, i).start()

        return 0

    lax.fori_loop(0, chunks, gather_state, 0)
    for load in loads[early:]:
        load.wait()
    for g in range(groups):
        cols = slice(g * state, (g + 1) * state)
        cc[:, cols] = conv(c, ec, kc, cols).astype(bf16)
        scores = jnp.dot(cc[:, cols], bt[g], preferred_element_type=f32)
        sc[g] = jnp.where(causal, scores, 0.0)
    per_tile = lanes // head_dim

    def finish(k, _):
        cols = pl.ds(pl.multiple_of(k * chunk, chunk), chunk)
        g = k // group_chunks
        scores = sc[g]
        columns_of = ldcol[k]
        for j in range(chunk // lanes):
            tile = pl.ds(pl.multiple_of(k * chunk + j * lanes, lanes), lanes)
            x_tile = xc[:, tile]
            lane = lax.broadcasted_iota(jnp.int32, (length, lanes), 1)
            inside = None
            for i in range(per_tile):
                n = j * per_tile + i
                h = k * per_chunk + n
                gap = columns_of[:, n : n + 1] - ldrow[pl.ds(h, 1), :]
                damping = jnp.exp(jnp.minimum(gap, 0.0))
                weights = (damping * steprow[pl.ds(h, 1), :] * scores).astype(bf16)
                term = jnp.dot(weights, x_tile, preferred_element_type=f32)
                inside = term if i == 0 else jnp.where(lane >= i * head_dim, term, inside)
            acc[:, tile] = inside

        @pl.when(me > 0)
        def _():
            for i in range(pieces):
                hand_on(k, i).wait_recv()
                some = pl.ds(pl.multiple_of(k * chunk + i * piece, piece), piece)

                @pl.when(jnp.logical_not(last))
                def _():
                    old = eld[length - 1 : length, some] * inbox[k, i].astype(f32)
                    outbox[k, i] = (old + sums[:, some]).astype(bf16)
                    hand_on(k, i).start()

            c_group = cc[:, pl.ds(pl.multiple_of(g * state, state), state)]
            for i in range(pieces):
                some = pl.ds(pl.multiple_of(k * chunk + i * piece, piece), piece)
                outside = jnp.dot(c_group, inbox[k, i], preferred_element_type=f32)
                acc[:, some] = acc[:, some] + outside * eld[:length, some]

        z_here = z[:, cols].astype(f32)
        total = acc[:, cols] + eld[length : length + 1, cols] * xc[:, cols].astype(f32)
        gated = total * (z_here * jax.nn.sigmoid(z_here))
        acc[:, cols] = gated
        square = gated * gated
        part = square[:, :lanes]
        for j in range(1, chunk // lanes):
            part = part + square[:, j * lanes : (j + 1) * lanes]
        ssq[...] = jnp.where(lax.rem(k, group_chunks) == 0, part, ssq[...] + part)

        @pl.when(lax.rem(k, group_chunks) == group_chunks - 1)
        def _():
            mean = jnp.sum(ssq[...], axis=1, keepdims=True) / (group_chunks * chunk)
            scale = lax.rsqrt(mean + epsilon)
            for j in range(group_chunks):
                first_col = (k - group_chunks + 1 + j) * chunk
                here = pl.ds(pl.multiple_of(first_col, chunk), chunk)
                value = (acc[:, here] * scale * gain[:, here]).astype(bf16)
                for e in range(heads):
                    for q in range(halves):
                        row = (e * halves + q) * rows
                        got[me * halves + q, e * rows : (e + 1) * rows, here] = value[row : row + rows]

        return 0

    lax.fori_loop(0, chunks, finish, 0)

    def gather(shard, peer, q):
        v = shard * halves + q
        return pltpu.make_async_remote_copy(
            got.at[v], got.at[v], ag_send.at[peer * halves + q], ag_recv.at[v],
            device_id={"seq": peer},
        )

    def send_up(v, e):
        return pltpu.make_async_remote_copy(
            part.at[v, e], up.at[v, e], u_send.at[v, e], u_recv.at[v, e],
            device_id={"head": h_z + 1},
        )

    def send_down(v, e):
        return pltpu.make_async_remote_copy(
            part.at[v, e], down.at[v, e], d_send.at[v, e], d_recv.at[v, e],
            device_id={"head": h_z - 1},
        )

    def deliver(peer, source, q):
        rows_out = pl.ds(pl.multiple_of(q * rows, rows), rows)
        columns = pl.ds(pl.multiple_of(source * width, width), width)
        return pltpu.make_async_remote_copy(
            part.at[peer * halves + q, h_z], out.at[rows_out, columns],
            o_send.at[peer * halves + q], o_recv.at[source * halves + q],
            device_id={"section": other, "seq": peer},
        )

    for d in range(1, shards):
        for q in range(halves):
            gather(me, partner(me, d, shards), q).start()

    def multiply(v):
        def one(i, _):
            cols = pl.ds(pl.multiple_of(i * tile, tile), tile)
            terms = jnp.dot(got[v], w_buf[:, cols], preferred_element_type=f32)
            part[v, :, :, cols] = terms.astype(bf16).reshape(heads, rows, tile)
            return 0

        lax.fori_loop(0, tiles, one, 0)

    steps = units * heads

    def decode(t):
        t = jnp.where(t < 0, 0, jnp.where(t < steps, t, steps - 1))
        d, r = t // (heads * halves), t % (heads * halves)
        return partner(me, d, shards), r % halves, r // halves

    def slot(t, _):
        shard, q, k = decode(t)

        @pl.when((t < steps) & (k == 0))
        def _():
            @pl.when(shard != me)
            def _():
                gather(shard, shard, q).wait_recv()

            multiply(shard * halves + q)

        t_up = t - h_z * lag
        shard_u, q_u, k_u = decode(t_up)

        @pl.when((t_up >= 0) & (t_up < steps))
        def _():
            v = shard_u * halves + q_u
            e = end - k_u

            @pl.when((e >= h_z) & (h_z > 0))
            def _():
                send_up(v, e).wait_recv()

            @pl.when((e > h_z) & (h_z > 0))
            def _():
                part[v, e] = (part[v, e].astype(f32) + up[v, e].astype(f32)).astype(bf16)

            @pl.when(e > h_z)
            def _():
                send_up(v, e).start()

        t_down = t - (end - h_z) * lag
        shard_d, q_d, k_d = decode(t_down)

        @pl.when((t_down >= 0) & (t_down < steps))
        def _():
            v = shard_d * halves + q_d

            @pl.when((k_d <= h_z) & (h_z < end))
            def _():
                send_down(v, k_d).wait_recv()

            @pl.when((k_d < h_z) & (h_z < end))
            def _():
                part[v, k_d] = (part[v, k_d].astype(f32) + down[v, k_d].astype(f32)).astype(bf16)

            @pl.when(k_d < h_z)
            def _():
                send_down(v, k_d).start()

        far = jnp.where(2 * h_z > end, h_z, end - h_z)
        t_last = t - far * lag
        shard_l, q_l, k_l = decode(t_last)

        @pl.when((t_last >= 0) & (t_last < steps) & (k_l == far))
        def _():
            v = shard_l * halves + q_l

            @pl.when(h_z == 0)
            def _():
                part[v, h_z] = (part[v, h_z].astype(f32) + down[v, h_z].astype(f32)).astype(bf16)

            @pl.when(h_z == end)
            def _():
                part[v, h_z] = (part[v, h_z].astype(f32) + up[v, h_z].astype(f32)).astype(bf16)

            @pl.when((h_z > 0) & (h_z < end))
            def _():
                total = part[v, h_z].astype(f32) + up[v, h_z].astype(f32)
                part[v, h_z] = (total + down[v, h_z].astype(f32)).astype(bf16)

            deliver(shard_l, here_s, q_l).start()

        return 0

    for load in w_loads:
        load.wait()
    lax.fori_loop(0, steps + end * lag, slot, 0)

    def drain(v, _):
        shard, q = v // halves, v % halves

        @pl.when(shard != me)
        def _():
            gather(me, shard, q).wait_send()

        for e in range(heads):

            @pl.when(e > h_z)
            def _():
                send_up(v, e).wait_send()

            @pl.when(e < h_z)
            def _():
                send_down(v, e).wait_send()

        deliver(shard, here_s, q).wait_send()
        deliver(here_s, shard, q).wait_recv()
        return 0

    lax.fori_loop(0, units, drain, 0)

    @pl.when(jnp.logical_not(last))
    def _():
        for copy in edges:
            copy.wait_send()

        def drain(k, _):
            for i in range(pieces):
                hand_on(k, i).wait_send()
            return 0

        lax.fori_loop(0, chunks, drain, 0)


def layer(args, weight, sizes):
    x, b, c, z, dt, kx, kb, kc, a, bias, skip, gain = args
    sections, shards, heads = sizes
    length, inner = x.shape
    depth, width = weight.shape
    head_count = dt.shape[0]
    head_dim = inner // head_count
    groups = b.shape[1] // N
    chunk, lanes, edge, halves, lag = 256, 128, 8, 2, 3
    chunks = inner // chunk
    count, units = length // halves, halves * shards
    rows = count // heads
    tile = min(512, width)
    f32, bf16 = jnp.float32, jnp.bfloat16
    dma = pltpu.SemaphoreType.DMA
    vmem = pltpu.VMEM
    return pl.pallas_call(
        functools.partial(layer_kernel, sizes, (head_dim, chunk, halves, lag)),
        out_shape=jax.ShapeDtypeStruct((halves * rows, shards * width), bf16),
        in_specs=[pl.BlockSpec(memory_space=pl.ANY)] * 13,
        out_specs=pl.BlockSpec(memory_space=pl.ANY),
        scratch_shapes=[vmem(array.shape, array.dtype) for array in args]
        + [
            dma((12,)),
            vmem((edge, inner), bf16),
            vmem((edge, b.shape[1]), bf16),
            vmem((edge, b.shape[1]), bf16),
            vmem((edge + length, chunk), f32),
            vmem((length, inner), bf16),
            vmem((groups, N, length), bf16),
            vmem((length, groups * N), bf16),
            vmem((groups, length, length), f32),
            vmem((24, lanes), f32),
            vmem((lanes, length), f32),
            vmem((lanes, length), f32),
            vmem((lanes, length), f32),
            vmem((chunks, length, chunk // head_dim), f32),
            vmem((length + 16, 2 * lanes), bf16),
            vmem((length, 2 * lanes), bf16),
            vmem((length + 16, inner), f32),
            vmem((N, inner), f32),
            vmem((length, inner), f32),
            vmem((length, lanes), f32),
            vmem((chunks, chunk // lanes, N, lanes), bf16),
            vmem((chunks, chunk // lanes, N, lanes), bf16),
            dma((3,)),
            dma((3,)),
            dma((chunks, chunk // lanes)),
            dma((chunks, chunk // lanes)),
            vmem(weight.shape, bf16),
            vmem((units, count, depth), bf16),
            vmem((units, heads, rows, width), bf16),
            vmem((units, heads, rows, width), bf16),
            vmem((units, heads, rows, width), bf16),
            dma((width // tile,)),
            dma((units,)),
            dma((units,)),
            dma((units, heads)),
            dma((units, heads)),
            dma((units, heads)),
            dma((units, heads)),
            dma((units,)),
            dma((units,)),
        ],
        compiler_params=pltpu.CompilerParams(
            collective_id=0, has_side_effects=True, vmem_limit_bytes=63 * 2**20
        ),
        cost_estimate=pl.CostEstimate(
            flops=2 * length * shards * depth * width,
            bytes_accessed=2 * weight.size,
            transcendentals=0,
        ),
        name="layer",
    )(*args, weight)


def per_device(
    x_in,
    b_in,
    c_in,
    z_in,
    dt_raw,
    conv_x,
    conv_b,
    conv_c,
    a_rate,
    dt_bias,
    skip_d,
    norm_gain,
    out_weight,
):
    sizes = tuple(lax.axis_size(name) for name in ("section", "seq", "head"))
    whole = (x_in, b_in, c_in, z_in, dt_raw, conv_x, conv_b, conv_c)
    args = [array[0] for array in whole] + [a_rate, dt_bias, skip_d, norm_gain]
    return layer(args, out_weight[0], sizes)[None]


def solution(mesh):
    return jax.shard_map(
        per_device,
        mesh=mesh,
        in_specs=(
            P("section", "seq", "head"),
            P("section", "seq", "head"),
            P("section", "seq", "head"),
            P("section", "seq", "head"),
            P("section", "head", "seq"),
            P("section", None, "head"),
            P("section", None, "head"),
            P("section", None, "head"),
            P("section", "head"),
            P("section", "head"),
            P("section", "head"),
            P("section", "head"),
            P("section", "head", "seq"),
        ),
        out_specs=P("section", ("seq", "head"), None),
        check_vma=False,
    )
```

```python
import functools

import jax
import jax.numpy as jnp
from jax import lax
from jax.experimental import pallas as pl
from jax.experimental.pallas import tpu as pltpu
from jax.sharding import PartitionSpec as P

N = 256


epsilon = 1e-05


def partner(place, bits, size):
    bit = 1
    while bit < size:
        flip = (bits // bit) % 2
        place = place + flip * (bit - 2 * bit * ((place // bit) % 2))
        bit *= 2
    return place


def layer_kernel(
    sizes, dims, x_hbm, b_hbm, c_hbm, z_hbm, dt_hbm, kx_hbm, kb_hbm, kc_hbm, a_hbm, bias_hbm,
    skip_hbm, gain_hbm, weight, out, x, b, c, z, dt, kx, kb, kc, a, bias, skip, gain, loaded,
    ex, eb, ec, pad, xc, bt, cc, sc, vec, dtp, ldrow, steprow, ldcol, cat, tocat,
    eld, sums, acc, gate, keep, ssq, inbox, outbox, e_send, e_recv, send, recv,
    w_buf, got, part, up, down,
    w_sem, ag_send, ag_recv, u_send, u_recv, d_send, d_recv, o_send, o_recv,
):
    sections, shards, heads = sizes
    head_dim, chunk, halves, lag = dims
    count = got.shape[1]
    units = shards * halves
    rows, width = part.shape[2], part.shape[3]
    tile = min(512, width)
    tiles = width // tile
    f32, bf16 = jnp.float32, jnp.bfloat16
    here_s, h_z = lax.axis_index("seq"), lax.axis_index("head")
    end = heads - 1
    other = lax.rem(lax.axis_index("section") + 1, sections)
    me = here_s
    length, inner = x.shape
    head_count = dt.shape[0]
    groups = sc.shape[0]
    state = bt.shape[1]
    taps = kx.shape[0]
    edge = ex.shape[0]
    chunks = inner // chunk
    per_chunk = chunk // head_dim
    group_chunks = chunks // groups
    lanes = 128
    after, before = lax.rem(me + 1, shards), lax.rem(me + shards - 1, shards)
    first, last = me == 0, me == shards - 1
    froms = (dt_hbm, a_hbm, bias_hbm, skip_hbm, kb_hbm, kx_hbm, b_hbm, x_hbm)
    tos = (dt, a, bias, skip, kb, kx, b, x)
    small, early = 4, len(tos)
    froms, tos = froms + (kc_hbm, c_hbm, z_hbm, gain_hbm), tos + (kc, c, z, gain)
    loads = [
        pltpu.make_async_copy(src, dst, loaded.at[n])
        for n, (src, dst) in enumerate(zip(froms, tos))
    ]
    for load in loads:
        load.start()
    w_loads = [
        pltpu.make_async_copy(
            weight.at[:, pl.ds(i * tile, tile)], w_buf.at[:, pl.ds(i * tile, tile)], w_sem.at[i]
        )
        for i in range(tiles)
    ]
    barrier = pltpu.get_barrier_semaphore()
    for d in range(shards):
        peer = partner(here_s, d, shards)
        if d:
            pl.semaphore_signal(barrier, inc=1, device_id={"seq": peer})
        pl.semaphore_signal(barrier, inc=1, device_id={"section": other, "seq": peer})

    @pl.when(h_z > 0)
    def _():
        pl.semaphore_signal(barrier, inc=1, device_id={"head": h_z - 1})

    @pl.when(h_z < end)
    def _():
        pl.semaphore_signal(barrier, inc=1, device_id={"head": h_z + 1})

    near = jnp.where(h_z > 0, 1, 0) + jnp.where(h_z < end, 1, 0)
    pl.semaphore_wait(barrier, 2 * shards - 1 + near)

    edges = [
        pltpu.make_async_remote_copy(
            src.at[pl.ds(length - edge, edge)], dst, e_send.at[n], e_recv.at[n],
            device_id={"seq": after},
        )
        for n, (src, dst) in enumerate(((x_hbm, ex), (b_hbm, eb), (c_hbm, ec)))
    ]

    pieces, slices = outbox.shape[1:3]
    piece = outbox.shape[4]
    deep = state // slices

    def hand_on(k, i, j):
        return pltpu.make_async_remote_copy(
            outbox.at[k, i, j], inbox.at[k, i, j], send.at[k, i, j], recv.at[k, i, j],
            device_id={"seq": after},
        )

    @pl.when(jnp.logical_not(last))
    def _():
        for copy in edges:
            copy.start()

    @pl.when(first)
    def _():
        for dst in (ex, eb, ec):
            dst[...] = jnp.zeros(dst.shape, dst.dtype)

    for load in loads[:small]:
        load.wait()

    vec[...] = jnp.zeros(vec.shape, f32)
    dtp[...] = jnp.zeros(dtp.shape, f32)
    dtp[:head_count, :] = dt[...]
    for n, ref in enumerate((a, bias, skip)):
        vec[8 * n : 8 * n + 1, :head_count] = ref[...]
    step = jax.nn.softplus(dtp[...].T + vec[8:9, :])
    causal = lax.broadcasted_iota(jnp.int32, (length, length), 0) >= lax.broadcasted_iota(
        jnp.int32, (length, length), 1
    )
    below = jnp.where(causal, 1.0, 0.0).astype(bf16)
    rest = -vec[0:1, :] * step
    decay = jnp.zeros((length, lanes), f32)
    for _ in range(3):
        high = rest.astype(bf16)
        decay = decay + jnp.dot(below, high, preferred_element_type=f32)
        rest = rest - high.astype(f32)
    keep[0] = decay
    keep[1] = step

    def split(dst, value, first_row):
        size = value.shape[0]
        high = value.astype(bf16)
        dst[first_row : first_row + size, :lanes] = high
        dst[first_row : first_row + size, lanes:] = (value - high.astype(f32)).astype(bf16)

    split(tocat, jnp.exp(decay[length - 1 : length, :] - decay) * step, 0)

    for load in loads[small:early]:
        load.wait()
    for load in w_loads:
        load.start()

    def conv(src, border, kernel, cols):
        pad[0:edge, :] = border[:, cols].astype(f32)
        pad[edge:, :] = src[:, cols].astype(f32)
        total = jnp.zeros((length, pad.shape[1]), f32)
        for k in range(taps):
            start = edge - taps + 1 + k
            total = total + kernel[k : k + 1, cols] * pad[start : start + length, :]
        return total * jax.nn.sigmoid(total)

    @pl.when(me > 0)
    def _():
        for copy in edges:
            copy.wait_recv()

    def ready(g):
        cols = pl.ds(pl.multiple_of(g * state, state), state)
        bt[g] = conv(b, eb, kb, cols).astype(bf16).astype(f32).T.astype(bf16)

    def spread(src, k):
        head = lax.broadcasted_iota(jnp.int32, (lanes, chunk), 0) - k * per_chunk
        lane = lax.broadcasted_iota(jnp.int32, (lanes, chunk), 1)
        start = head * head_dim
        pick = jnp.where((lane >= start) & (lane < start + head_dim), 1.0, 0.0).astype(bf16)
        pick = jnp.concatenate([pick, pick], axis=0)
        return jnp.dot(src[...], pick, preferred_element_type=f32)

    def gather_state(k, _):
        @pl.when(lax.rem(k, group_chunks) == 0)
        def _():
            ready(k // group_chunks)

        cols = pl.ds(pl.multiple_of(k * chunk, chunk), chunk)
        x_conv = conv(x, ex, kx, cols).astype(bf16)
        xc[:, cols] = x_conv
        weighted = (x_conv.astype(f32) * spread(tocat, k)).astype(bf16)
        total = jnp.dot(bt[k // group_chunks], weighted, preferred_element_type=f32)
        sums[:, cols] = total

        @pl.when(first)
        def _():
            for i in range(pieces):
                for j in range(slices):
                    some = total[j * deep : (j + 1) * deep, i * piece : (i + 1) * piece]
                    outbox[k, i, j] = some.astype(bf16)
                    hand_on(k, i, j).start()

        return 0

    lax.fori_loop(0, chunks, gather_state, 0)
    for load in loads[early:]:
        load.wait()
    decay = keep[0]
    ldrow[...] = decay.T
    steprow[...] = keep[1].T
    for k in range(chunks):
        ldcol[k] = decay[:, k * per_chunk : (k + 1) * per_chunk]
    split(cat, jnp.exp(decay), 0)
    split(cat, jnp.broadcast_to(vec[16:17, :], (16, lanes)), length)
    for g in range(groups):
        cols = slice(g * state, (g + 1) * state)
        cc[:, cols] = conv(c, ec, kc, cols).astype(bf16)
        scores = jnp.dot(cc[:, cols], bt[g], preferred_element_type=f32)
        sc[g] = jnp.where(causal, scores, 0.0)
    per_tile = lanes // head_dim

    def finish(k, _):
        cols = pl.ds(pl.multiple_of(k * chunk, chunk), chunk)
        g = k // group_chunks
        eld[:, cols] = spread(cat, k)
        z_here = z[:, cols].astype(f32)
        gate[...] = z_here * jax.nn.sigmoid(z_here)
        scores = sc[g]
        columns_of = ldcol[k]
        for j in range(chunk // lanes):
            tile = pl.ds(pl.multiple_of(k * chunk + j * lanes, lanes), lanes)
            x_tile = xc[:, tile]
            lane = lax.broadcasted_iota(jnp.int32, (length, lanes), 1)
            inside = None
            for i in range(per_tile):
                n = j * per_tile + i
                h = k * per_chunk + n
                gap = columns_of[:, n : n + 1] - ldrow[pl.ds(h, 1), :]
                damping = jnp.exp(jnp.minimum(gap, 0.0))
                weights = (damping * steprow[pl.ds(h, 1), :] * scores).astype(bf16)
                term = jnp.dot(weights, x_tile, preferred_element_type=f32)
                inside = term if i == 0 else jnp.where(lane >= i * head_dim, term, inside)
            acc[:, tile] = inside + eld[length : length + 1, tile] * x_tile.astype(f32)

        @pl.when(me > 0)
        def _():
            for i in range(pieces):
                some = pl.ds(pl.multiple_of(k * chunk + i * piece, piece), piece)
                for j in range(slices):
                    hand_on(k, i, j).wait_recv()

                    @pl.when(jnp.logical_not(last))
                    def _():
                        old = eld[length - 1 : length, some] * inbox[k, i, j].astype(f32)
                        new = old + sums[j * deep : (j + 1) * deep, some]
                        outbox[k, i, j] = new.astype(bf16)
                        hand_on(k, i, j).start()

            c_group = cc[:, pl.ds(pl.multiple_of(g * state, state), state)]
            for i in range(pieces):
                some = pl.ds(pl.multiple_of(k * chunk + i * piece, piece), piece)
                here = inbox[k, i].reshape(state, piece)
                outside = jnp.dot(c_group, here, preferred_element_type=f32)
                acc[:, some] = acc[:, some] + outside * eld[:length, some]

        gated = acc[:, cols] * gate[...]
        acc[:, cols] = gated
        square = gated * gated
        part = square[:, :lanes]
        for j in range(1, chunk // lanes):
            part = part + square[:, j * lanes : (j + 1) * lanes]
        ssq[...] = jnp.where(lax.rem(k, group_chunks) == 0, part, ssq[...] + part)

        @pl.when(lax.rem(k, group_chunks) == group_chunks - 1)
        def _():
            mean = jnp.sum(ssq[...], axis=1, keepdims=True) / (group_chunks * chunk)
            scale = lax.rsqrt(mean + epsilon)
            for j in range(group_chunks):
                first_col = (k - group_chunks + 1 + j) * chunk
                here = pl.ds(pl.multiple_of(first_col, chunk), chunk)
                value = (acc[:, here] * scale * gain[:, here]).astype(bf16)
                for e in range(heads):
                    for q in range(halves):
                        row = (e * halves + q) * rows
                        got[me * halves + q, e * rows : (e + 1) * rows, here] = value[row : row + rows]

        return 0

    lax.fori_loop(0, chunks, finish, 0)

    def gather(shard, peer, q):
        v = shard * halves + q
        return pltpu.make_async_remote_copy(
            got.at[v], got.at[v], ag_send.at[peer * halves + q], ag_recv.at[v],
            device_id={"seq": peer},
        )

    def send_up(v, e):
        return pltpu.make_async_remote_copy(
            part.at[v, e], up.at[v, e], u_send.at[v, e], u_recv.at[v, e],
            device_id={"head": h_z + 1},
        )

    def send_down(v, e):
        return pltpu.make_async_remote_copy(
            part.at[v, e], down.at[v, e], d_send.at[v, e], d_recv.at[v, e],
            device_id={"head": h_z - 1},
        )

    def deliver(peer, source, q):
        rows_out = pl.ds(pl.multiple_of(q * rows, rows), rows)
        columns = pl.ds(pl.multiple_of(source * width, width), width)
        return pltpu.make_async_remote_copy(
            part.at[peer * halves + q, h_z], out.at[rows_out, columns],
            o_send.at[peer * halves + q], o_recv.at[source * halves + q],
            device_id={"section": other, "seq": peer},
        )

    def spread_rows(distances):
        for d in distances:
            for q in range(halves):
                gather(me, partner(me, d, shards), q).start()

    spread_rows(range(1, min(3, shards)))

    def multiply(v):
        def one(i, _):
            cols = pl.ds(pl.multiple_of(i * tile, tile), tile)
            terms = jnp.dot(got[v], w_buf[:, cols], preferred_element_type=f32)
            part[v, :, :, cols] = terms.astype(bf16).reshape(heads, rows, tile)
            return 0

        lax.fori_loop(0, tiles, one, 0)

    steps = units * heads

    def decode(t):
        t = jnp.where(t < 0, 0, jnp.where(t < steps, t, steps - 1))
        d, r = t // (heads * halves), t % (heads * halves)
        return partner(me, d, shards), r % halves, r // halves

    def slot(t, _):
        @pl.when(t == 2 * heads * halves)
        def _():
            spread_rows(range(3, shards))

        shard, q, k = decode(t)

        @pl.when((t < steps) & (k == 0))
        def _():
            @pl.when(shard != me)
            def _():
                gather(shard, shard, q).wait_recv()

            multiply(shard * halves + q)

        t_up = t - h_z * lag
        shard_u, q_u, k_u = decode(t_up)

        @pl.when((t_up >= 0) & (t_up < steps))
        def _():
            v = shard_u * halves + q_u
            e = end - k_u

            @pl.when((e >= h_z) & (h_z > 0))
            def _():
                send_up(v, e).wait_recv()

            @pl.when((e > h_z) & (h_z > 0))
            def _():
                part[v, e] = (part[v, e].astype(f32) + up[v, e].astype(f32)).astype(bf16)

            @pl.when(e > h_z)
            def _():
                send_up(v, e).start()

        t_down = t - (end - h_z) * lag
        shard_d, q_d, k_d = decode(t_down)

        @pl.when((t_down >= 0) & (t_down < steps))
        def _():
            v = shard_d * halves + q_d

            @pl.when((k_d <= h_z) & (h_z < end))
            def _():
                send_down(v, k_d).wait_recv()

            @pl.when((k_d < h_z) & (h_z < end))
            def _():
                part[v, k_d] = (part[v, k_d].astype(f32) + down[v, k_d].astype(f32)).astype(bf16)

            @pl.when(k_d < h_z)
            def _():
                send_down(v, k_d).start()

        far = jnp.where(2 * h_z > end, h_z, end - h_z)
        t_last = t - far * lag
        shard_l, q_l, k_l = decode(t_last)

        @pl.when((t_last >= 0) & (t_last < steps) & (k_l == far))
        def _():
            v = shard_l * halves + q_l

            @pl.when(h_z == 0)
            def _():
                part[v, h_z] = (part[v, h_z].astype(f32) + down[v, h_z].astype(f32)).astype(bf16)

            @pl.when(h_z == end)
            def _():
                part[v, h_z] = (part[v, h_z].astype(f32) + up[v, h_z].astype(f32)).astype(bf16)

            @pl.when((h_z > 0) & (h_z < end))
            def _():
                total = part[v, h_z].astype(f32) + up[v, h_z].astype(f32)
                part[v, h_z] = (total + down[v, h_z].astype(f32)).astype(bf16)

            deliver(shard_l, here_s, q_l).start()

        return 0

    for load in w_loads:
        load.wait()
    lax.fori_loop(0, steps + end * lag, slot, 0)

    def drain(v, _):
        shard, q = v // halves, v % halves

        @pl.when(shard != me)
        def _():
            gather(me, shard, q).wait_send()

        for e in range(heads):

            @pl.when(e > h_z)
            def _():
                send_up(v, e).wait_send()

            @pl.when(e < h_z)
            def _():
                send_down(v, e).wait_send()

        deliver(shard, here_s, q).wait_send()
        deliver(here_s, shard, q).wait_recv()
        return 0

    lax.fori_loop(0, units, drain, 0)

    @pl.when(jnp.logical_not(last))
    def _():
        for copy in edges:
            copy.wait_send()

        def drain(k, _):
            for i in range(pieces):
                for j in range(slices):
                    hand_on(k, i, j).wait_send()
            return 0

        lax.fori_loop(0, chunks, drain, 0)


def layer(args, weight, sizes):
    x, b, c, z, dt, kx, kb, kc, a, bias, skip, gain = args
    sections, shards, heads = sizes
    length, inner = x.shape
    depth, width = weight.shape
    head_count = dt.shape[0]
    head_dim = inner // head_count
    groups = b.shape[1] // N
    chunk, lanes, edge, halves, lag = 256, 128, 8, 2, 3
    chunks, slices = inner // chunk, 1
    count, units = length // halves, halves * shards
    rows = count // heads
    tile = min(512, width)
    f32, bf16 = jnp.float32, jnp.bfloat16
    dma = pltpu.SemaphoreType.DMA
    vmem = pltpu.VMEM
    return pl.pallas_call(
        functools.partial(layer_kernel, sizes, (head_dim, chunk, halves, lag)),
        out_shape=jax.ShapeDtypeStruct((halves * rows, shards * width), bf16),
        in_specs=[pl.BlockSpec(memory_space=pl.ANY)] * 13,
        out_specs=pl.BlockSpec(memory_space=pl.ANY),
        scratch_shapes=[vmem(array.shape, array.dtype) for array in args]
        + [
            dma((12,)),
            vmem((edge, inner), bf16),
            vmem((edge, b.shape[1]), bf16),
            vmem((edge, b.shape[1]), bf16),
            vmem((edge + length, chunk), f32),
            vmem((length, inner), bf16),
            vmem((groups, N, length), bf16),
            vmem((length, groups * N), bf16),
            vmem((groups, length, length), f32),
            vmem((24, lanes), f32),
            vmem((lanes, length), f32),
            vmem((lanes, length), f32),
            vmem((lanes, length), f32),
            vmem((chunks, length, chunk // head_dim), f32),
            vmem((length + 16, 2 * lanes), bf16),
            vmem((length, 2 * lanes), bf16),
            vmem((length + 16, inner), f32),
            vmem((N, inner), f32),
            vmem((length, inner), f32),
            vmem((length, chunk), f32),
            vmem((2, length, lanes), f32),
            vmem((length, lanes), f32),
            vmem((chunks, chunk // lanes, slices, N // slices, lanes), bf16),
            vmem((chunks, chunk // lanes, slices, N // slices, lanes), bf16),
            dma((3,)),
            dma((3,)),
            dma((chunks, chunk // lanes, slices)),
            dma((chunks, chunk // lanes, slices)),
            vmem(weight.shape, bf16),
            vmem((units, count, depth), bf16),
            vmem((units, heads, rows, width), bf16),
            vmem((units, heads, rows, width), bf16),
            vmem((units, heads, rows, width), bf16),
            dma((width // tile,)),
            dma((units,)),
            dma((units,)),
            dma((units, heads)),
            dma((units, heads)),
            dma((units, heads)),
            dma((units, heads)),
            dma((units,)),
            dma((units,)),
        ],
        compiler_params=pltpu.CompilerParams(
            collective_id=0, has_side_effects=True, vmem_limit_bytes=63 * 2**20
        ),
        cost_estimate=pl.CostEstimate(
            flops=2 * length * shards * depth * width,
            bytes_accessed=2 * weight.size,
            transcendentals=0,
        ),
        name="layer",
    )(*args, weight)


def per_device(
    x_in,
    b_in,
    c_in,
    z_in,
    dt_raw,
    conv_x,
    conv_b,
    conv_c,
    a_rate,
    dt_bias,
    skip_d,
    norm_gain,
    out_weight,
):
    sizes = tuple(lax.axis_size(name) for name in ("section", "seq", "head"))
    whole = (x_in, b_in, c_in, z_in, dt_raw, conv_x, conv_b, conv_c)
    args = [array[0] for array in whole] + [a_rate, dt_bias, skip_d, norm_gain]
    return layer(args, out_weight[0], sizes)[None]


def solution(mesh):
    return jax.shard_map(
        per_device,
        mesh=mesh,
        in_specs=(
            P("section", "seq", "head"),
            P("section", "seq", "head"),
            P("section", "seq", "head"),
            P("section", "seq", "head"),
            P("section", "head", "seq"),
            P("section", None, "head"),
            P("section", None, "head"),
            P("section", None, "head"),
            P("section", "head"),
            P("section", "head"),
            P("section", "head"),
            P("section", "head"),
            P("section", "head", "seq"),
        ),
        out_specs=P("section", ("seq", "head"), None),
        check_vma=False,
    )
```

```python
import functools

import jax
import jax.numpy as jnp
from jax import lax
from jax.experimental import pallas as pl
from jax.experimental.pallas import tpu as pltpu
from jax.sharding import PartitionSpec as P

N = 256


epsilon = 1e-05


def partner(place, bits, size):
    bit = 1
    while bit < size:
        flip = (bits // bit) % 2
        place = place + flip * (bit - 2 * bit * ((place // bit) % 2))
        bit *= 2
    return place


def layer_kernel(
    sizes, dims, x_hbm, b_hbm, c_hbm, z_hbm, dt_hbm, kx_hbm, kb_hbm, kc_hbm, a_hbm, bias_hbm,
    skip_hbm, gain_hbm, weight, out, x, b, c, z, dt, kx, kb, kc, a, bias, skip, gain, loaded,
    ex, eb, ec, pad, xc, bt, cc, sc, vec, dtp, ldrow, steprow, ldcol, cat, tocat,
    eld, sums, acc, gate, keep, ssq, inbox, outbox, e_send, e_recv, send, recv,
    w_buf, got, part, up, down,
    w_sem, ag_send, ag_recv, u_send, u_recv, d_send, d_recv, o_send, o_recv,
):
    sections, shards, heads = sizes
    head_dim, chunk, halves, lag = dims
    count = got.shape[1]
    units = shards * halves
    rows, width = part.shape[2], part.shape[3]
    tile = min(1024, width)
    tiles = width // tile
    f32, bf16 = jnp.float32, jnp.bfloat16
    here_s, h_z = lax.axis_index("seq"), lax.axis_index("head")
    end = heads - 1
    other = lax.rem(lax.axis_index("section") + 1, sections)
    me = here_s
    length, inner = x.shape
    head_count = dt.shape[0]
    groups = sc.shape[0]
    state = bt.shape[1]
    taps = kx.shape[0]
    edge = ex.shape[0]
    chunks = inner // chunk
    per_chunk = chunk // head_dim
    group_chunks = chunks // groups
    lanes = 128
    after, before = lax.rem(me + 1, shards), lax.rem(me + shards - 1, shards)
    first, last = me == 0, me == shards - 1
    froms = (dt_hbm, a_hbm, bias_hbm, skip_hbm, kb_hbm, kx_hbm, b_hbm, x_hbm)
    tos = (dt, a, bias, skip, kb, kx, b, x)
    small, early = 4, len(tos)
    froms, tos = froms + (kc_hbm, c_hbm, z_hbm, gain_hbm), tos + (kc, c, z, gain)
    loads = [
        pltpu.make_async_copy(src, dst, loaded.at[n])
        for n, (src, dst) in enumerate(zip(froms, tos))
    ]
    for load in loads:
        load.start()
    w_loads = [
        pltpu.make_async_copy(
            weight.at[:, pl.ds(i * tile, tile)], w_buf.at[:, pl.ds(i * tile, tile)], w_sem.at[i]
        )
        for i in range(tiles)
    ]
    barrier = pltpu.get_barrier_semaphore()
    for d in range(shards):
        peer = partner(here_s, d, shards)
        if d:
            pl.semaphore_signal(barrier, inc=1, device_id={"seq": peer})
        pl.semaphore_signal(barrier, inc=1, device_id={"section": other, "seq": peer})

    @pl.when(h_z > 0)
    def _():
        pl.semaphore_signal(barrier, inc=1, device_id={"head": h_z - 1})

    @pl.when(h_z < end)
    def _():
        pl.semaphore_signal(barrier, inc=1, device_id={"head": h_z + 1})

    near = jnp.where(h_z > 0, 1, 0) + jnp.where(h_z < end, 1, 0)
    pl.semaphore_wait(barrier, 2 * shards - 1 + near)

    edges = [
        pltpu.make_async_remote_copy(
            src.at[pl.ds(length - edge, edge)], dst, e_send.at[n], e_recv.at[n],
            device_id={"seq": after},
        )
        for n, (src, dst) in enumerate(((x_hbm, ex), (b_hbm, eb), (c_hbm, ec)))
    ]

    pieces, slices = outbox.shape[1:3]
    piece = outbox.shape[4]
    deep = state // slices

    def hand_on(k, i, j):
        return pltpu.make_async_remote_copy(
            outbox.at[k, i, j], inbox.at[k, i, j], send.at[k, i, j], recv.at[k, i, j],
            device_id={"seq": after},
        )

    @pl.when(jnp.logical_not(last))
    def _():
        for copy in edges:
            copy.start()

    @pl.when(first)
    def _():
        for dst in (ex, eb, ec):
            dst[...] = jnp.zeros(dst.shape, dst.dtype)

    for load in loads[:small]:
        load.wait()

    vec[...] = jnp.zeros(vec.shape, f32)
    dtp[...] = jnp.zeros(dtp.shape, f32)
    dtp[:head_count, :] = dt[...]
    for n, ref in enumerate((a, bias, skip)):
        vec[8 * n : 8 * n + 1, :head_count] = ref[...]
    step = jax.nn.softplus(dtp[...].T + vec[8:9, :])
    causal = lax.broadcasted_iota(jnp.int32, (length, length), 0) >= lax.broadcasted_iota(
        jnp.int32, (length, length), 1
    )
    below = jnp.where(causal, 1.0, 0.0).astype(bf16)
    rest = -vec[0:1, :] * step
    decay = jnp.zeros((length, lanes), f32)
    for _ in range(3):
        high = rest.astype(bf16)
        decay = decay + jnp.dot(below, high, preferred_element_type=f32)
        rest = rest - high.astype(f32)
    keep[0] = decay
    keep[1] = step

    def split(dst, value, first_row):
        size = value.shape[0]
        high = value.astype(bf16)
        dst[first_row : first_row + size, :lanes] = high
        dst[first_row : first_row + size, lanes:] = (value - high.astype(f32)).astype(bf16)

    split(tocat, jnp.exp(decay[length - 1 : length, :] - decay) * step, 0)

    for load in loads[small:early]:
        load.wait()
    for load in w_loads:
        load.start()

    def conv(src, border, kernel, cols):
        pad[0:edge, :] = border[:, cols].astype(f32)
        pad[edge:, :] = src[:, cols].astype(f32)
        total = jnp.zeros((length, pad.shape[1]), f32)
        for k in range(taps):
            start = edge - taps + 1 + k
            total = total + kernel[k : k + 1, cols] * pad[start : start + length, :]
        return total * jax.nn.sigmoid(total)

    @pl.when(me > 0)
    def _():
        for copy in edges:
            copy.wait_recv()

    def ready(g):
        cols = pl.ds(pl.multiple_of(g * state, state), state)
        bt[g] = conv(b, eb, kb, cols).astype(bf16).astype(f32).T.astype(bf16)

    def spread(src, k):
        head = lax.broadcasted_iota(jnp.int32, (lanes, chunk), 0) - k * per_chunk
        lane = lax.broadcasted_iota(jnp.int32, (lanes, chunk), 1)
        start = head * head_dim
        pick = jnp.where((lane >= start) & (lane < start + head_dim), 1.0, 0.0).astype(bf16)
        pick = jnp.concatenate([pick, pick], axis=0)
        return jnp.dot(src[...], pick, preferred_element_type=f32)

    def gather_state(k, _):
        @pl.when(lax.rem(k, group_chunks) == 0)
        def _():
            ready(k // group_chunks)

        cols = pl.ds(pl.multiple_of(k * chunk, chunk), chunk)
        x_conv = conv(x, ex, kx, cols).astype(bf16)
        xc[:, cols] = x_conv
        weighted = (x_conv.astype(f32) * spread(tocat, k)).astype(bf16)
        total = jnp.dot(bt[k // group_chunks], weighted, preferred_element_type=f32)
        sums[:, cols] = total

        @pl.when(first)
        def _():
            for i in range(pieces):
                for j in range(slices):
                    some = total[j * deep : (j + 1) * deep, i * piece : (i + 1) * piece]
                    outbox[k, i, j] = some.astype(bf16)
                    hand_on(k, i, j).start()

        return 0

    lax.fori_loop(0, chunks, gather_state, 0)
    for load in loads[early:]:
        load.wait()
    decay = keep[0]
    ldrow[...] = decay.T
    steprow[...] = keep[1].T
    for k in range(chunks):
        ldcol[k] = decay[:, k * per_chunk : (k + 1) * per_chunk]
    split(cat, jnp.exp(decay), 0)
    split(cat, jnp.broadcast_to(vec[16:17, :], (16, lanes)), length)
    for g in range(groups):
        cols = slice(g * state, (g + 1) * state)
        cc[:, cols] = conv(c, ec, kc, cols).astype(bf16)
        scores = jnp.dot(cc[:, cols], bt[g], preferred_element_type=f32)
        sc[g] = jnp.where(causal, scores, 0.0)
    per_tile = lanes // head_dim

    def finish(k, _):
        cols = pl.ds(pl.multiple_of(k * chunk, chunk), chunk)
        g = k // group_chunks
        eld[:, cols] = spread(cat, k)
        z_here = z[:, cols].astype(f32)
        gate[...] = z_here * jax.nn.sigmoid(z_here)
        scores = sc[g]
        columns_of = ldcol[k]
        for j in range(chunk // lanes):
            tile = pl.ds(pl.multiple_of(k * chunk + j * lanes, lanes), lanes)
            x_tile = xc[:, tile]
            lane = lax.broadcasted_iota(jnp.int32, (length, lanes), 1)
            inside = None
            for i in range(per_tile):
                n = j * per_tile + i
                h = k * per_chunk + n
                gap = columns_of[:, n : n + 1] - ldrow[pl.ds(h, 1), :]
                damping = jnp.exp(jnp.minimum(gap, 0.0))
                weights = (damping * steprow[pl.ds(h, 1), :] * scores).astype(bf16)
                term = jnp.dot(weights, x_tile, preferred_element_type=f32)
                inside = term if i == 0 else jnp.where(lane >= i * head_dim, term, inside)
            acc[:, tile] = inside + eld[length : length + 1, tile] * x_tile.astype(f32)

        @pl.when(me > 0)
        def _():
            for i in range(pieces):
                some = pl.ds(pl.multiple_of(k * chunk + i * piece, piece), piece)
                for j in range(slices):
                    hand_on(k, i, j).wait_recv()

                    @pl.when(jnp.logical_not(last))
                    def _():
                        old = eld[length - 1 : length, some] * inbox[k, i, j].astype(f32)
                        new = old + sums[j * deep : (j + 1) * deep, some]
                        outbox[k, i, j] = new.astype(bf16)
                        hand_on(k, i, j).start()

            c_group = cc[:, pl.ds(pl.multiple_of(g * state, state), state)]
            for i in range(pieces):
                some = pl.ds(pl.multiple_of(k * chunk + i * piece, piece), piece)
                here = inbox[k, i].reshape(state, piece)
                outside = jnp.dot(c_group, here, preferred_element_type=f32)
                acc[:, some] = acc[:, some] + outside * eld[:length, some]

        gated = acc[:, cols] * gate[...]
        acc[:, cols] = gated
        square = gated * gated
        part = square[:, :lanes]
        for j in range(1, chunk // lanes):
            part = part + square[:, j * lanes : (j + 1) * lanes]
        ssq[...] = jnp.where(lax.rem(k, group_chunks) == 0, part, ssq[...] + part)

        @pl.when(lax.rem(k, group_chunks) == group_chunks - 1)
        def _():
            mean = jnp.sum(ssq[...], axis=1, keepdims=True) / (group_chunks * chunk)
            scale = lax.rsqrt(mean + epsilon)
            for j in range(group_chunks):
                first_col = (k - group_chunks + 1 + j) * chunk
                here = pl.ds(pl.multiple_of(first_col, chunk), chunk)
                value = (acc[:, here] * scale * gain[:, here]).astype(bf16)
                for e in range(heads):
                    for q in range(halves):
                        row = (e * halves + q) * rows
                        got[me * halves + q, e * rows : (e + 1) * rows, here] = value[row : row + rows]

        return 0

    lax.fori_loop(0, chunks, finish, 0)

    def gather(shard, peer, q):
        v = shard * halves + q
        return pltpu.make_async_remote_copy(
            got.at[v], got.at[v], ag_send.at[peer * halves + q], ag_recv.at[v],
            device_id={"seq": peer},
        )

    def send_up(v, e):
        return pltpu.make_async_remote_copy(
            part.at[v, e], up.at[v, e], u_send.at[v, e], u_recv.at[v, e],
            device_id={"head": h_z + 1},
        )

    def send_down(v, e):
        return pltpu.make_async_remote_copy(
            part.at[v, e], down.at[v, e], d_send.at[v, e], d_recv.at[v, e],
            device_id={"head": h_z - 1},
        )

    def deliver(peer, source, q):
        rows_out = pl.ds(pl.multiple_of(q * rows, rows), rows)
        columns = pl.ds(pl.multiple_of(source * width, width), width)
        return pltpu.make_async_remote_copy(
            part.at[peer * halves + q, h_z], out.at[rows_out, columns],
            o_send.at[peer * halves + q], o_recv.at[source * halves + q],
            device_id={"section": other, "seq": peer},
        )

    def spread_rows(distances):
        for d in distances:
            for q in range(halves):
                gather(me, partner(me, d, shards), q).start()

    spread_rows(range(1, min(3, shards)))

    def multiply(v):
        def one(i, _):
            cols = pl.ds(pl.multiple_of(i * tile, tile), tile)
            terms = jnp.dot(got[v], w_buf[:, cols], preferred_element_type=f32)
            part[v, :, :, cols] = terms.astype(bf16).reshape(heads, rows, tile)
            return 0

        lax.fori_loop(0, tiles, one, 0)

    steps = units * heads

    def decode(t):
        t = jnp.where(t < 0, 0, jnp.where(t < steps, t, steps - 1))
        d, r = t // (heads * halves), t % (heads * halves)
        return partner(me, d, shards), r % halves, r // halves

    def slot(t, _):
        @pl.when(t == 2 * heads * halves)
        def _():
            spread_rows(range(3, shards))

        shard, q, k = decode(t)

        @pl.when((t < steps) & (k == 0))
        def _():
            @pl.when(shard != me)
            def _():
                gather(shard, shard, q).wait_recv()

            multiply(shard * halves + q)

        t_up = t - h_z * lag
        shard_u, q_u, k_u = decode(t_up)

        @pl.when((t_up >= 0) & (t_up < steps))
        def _():
            v = shard_u * halves + q_u
            e = end - k_u

            @pl.when((e >= h_z) & (h_z > 0))
            def _():
                send_up(v, e).wait_recv()

            @pl.when((e > h_z) & (h_z > 0))
            def _():
                part[v, e] = (part[v, e].astype(f32) + up[v, e].astype(f32)).astype(bf16)

            @pl.when(e > h_z)
            def _():
                send_up(v, e).start()

        t_down = t - (end - h_z) * lag
        shard_d, q_d, k_d = decode(t_down)

        @pl.when((t_down >= 0) & (t_down < steps))
        def _():
            v = shard_d * halves + q_d

            @pl.when((k_d <= h_z) & (h_z < end))
            def _():
                send_down(v, k_d).wait_recv()

            @pl.when((k_d < h_z) & (h_z < end))
            def _():
                part[v, k_d] = (part[v, k_d].astype(f32) + down[v, k_d].astype(f32)).astype(bf16)

            @pl.when(k_d < h_z)
            def _():
                send_down(v, k_d).start()

        far = jnp.where(2 * h_z > end, h_z, end - h_z)
        t_last = t - far * lag
        shard_l, q_l, k_l = decode(t_last)

        @pl.when((t_last >= 0) & (t_last < steps) & (k_l == far))
        def _():
            v = shard_l * halves + q_l

            @pl.when(h_z == 0)
            def _():
                part[v, h_z] = (part[v, h_z].astype(f32) + down[v, h_z].astype(f32)).astype(bf16)

            @pl.when(h_z == end)
            def _():
                part[v, h_z] = (part[v, h_z].astype(f32) + up[v, h_z].astype(f32)).astype(bf16)

            @pl.when((h_z > 0) & (h_z < end))
            def _():
                total = part[v, h_z].astype(f32) + up[v, h_z].astype(f32)
                part[v, h_z] = (total + down[v, h_z].astype(f32)).astype(bf16)

            deliver(shard_l, here_s, q_l).start()

        return 0

    for load in w_loads:
        load.wait()
    lax.fori_loop(0, steps + end * lag, slot, 0)

    def drain(v, _):
        shard, q = v // halves, v % halves

        @pl.when(shard != me)
        def _():
            gather(me, shard, q).wait_send()

        for e in range(heads):

            @pl.when(e > h_z)
            def _():
                send_up(v, e).wait_send()

            @pl.when(e < h_z)
            def _():
                send_down(v, e).wait_send()

        deliver(shard, here_s, q).wait_send()
        deliver(here_s, shard, q).wait_recv()
        return 0

    lax.fori_loop(0, units, drain, 0)

    @pl.when(jnp.logical_not(last))
    def _():
        for copy in edges:
            copy.wait_send()

        def drain(k, _):
            for i in range(pieces):
                for j in range(slices):
                    hand_on(k, i, j).wait_send()
            return 0

        lax.fori_loop(0, chunks, drain, 0)


def layer(args, weight, sizes):
    x, b, c, z, dt, kx, kb, kc, a, bias, skip, gain = args
    sections, shards, heads = sizes
    length, inner = x.shape
    depth, width = weight.shape
    head_count = dt.shape[0]
    head_dim = inner // head_count
    groups = b.shape[1] // N
    chunk, lanes, edge, halves, lag = 256, 128, 8, 2, 3
    chunks, slices = inner // chunk, 1
    count, units = length // halves, halves * shards
    rows = count // heads
    tile = min(1024, width)
    f32, bf16 = jnp.float32, jnp.bfloat16
    dma = pltpu.SemaphoreType.DMA
    vmem = pltpu.VMEM
    return pl.pallas_call(
        functools.partial(layer_kernel, sizes, (head_dim, chunk, halves, lag)),
        out_shape=jax.ShapeDtypeStruct((halves * rows, shards * width), bf16),
        in_specs=[pl.BlockSpec(memory_space=pl.ANY)] * 13,
        out_specs=pl.BlockSpec(memory_space=pl.ANY),
        scratch_shapes=[vmem(array.shape, array.dtype) for array in args]
        + [
            dma((12,)),
            vmem((edge, inner), bf16),
            vmem((edge, b.shape[1]), bf16),
            vmem((edge, b.shape[1]), bf16),
            vmem((edge + length, chunk), f32),
            vmem((length, inner), bf16),
            vmem((groups, N, length), bf16),
            vmem((length, groups * N), bf16),
            vmem((groups, length, length), f32),
            vmem((24, lanes), f32),
            vmem((lanes, length), f32),
            vmem((lanes, length), f32),
            vmem((lanes, length), f32),
            vmem((chunks, length, chunk // head_dim), f32),
            vmem((length + 16, 2 * lanes), bf16),
            vmem((length, 2 * lanes), bf16),
            vmem((length + 16, inner), f32),
            vmem((N, inner), f32),
            vmem((length, inner), f32),
            vmem((length, chunk), f32),
            vmem((2, length, lanes), f32),
            vmem((length, lanes), f32),
            vmem((chunks, chunk // lanes, slices, N // slices, lanes), bf16),
            vmem((chunks, chunk // lanes, slices, N // slices, lanes), bf16),
            dma((3,)),
            dma((3,)),
            dma((chunks, chunk // lanes, slices)),
            dma((chunks, chunk // lanes, slices)),
            vmem(weight.shape, bf16),
            vmem((units, count, depth), bf16),
            vmem((units, heads, rows, width), bf16),
            vmem((units, heads, rows, width), bf16),
            vmem((units, heads, rows, width), bf16),
            dma((width // tile,)),
            dma((units,)),
            dma((units,)),
            dma((units, heads)),
            dma((units, heads)),
            dma((units, heads)),
            dma((units, heads)),
            dma((units,)),
            dma((units,)),
        ],
        compiler_params=pltpu.CompilerParams(
            collective_id=0, has_side_effects=True, vmem_limit_bytes=63 * 2**20
        ),
        cost_estimate=pl.CostEstimate(
            flops=2 * length * shards * depth * width,
            bytes_accessed=2 * weight.size,
            transcendentals=0,
        ),
        name="layer",
    )(*args, weight)


def per_device(
    x_in,
    b_in,
    c_in,
    z_in,
    dt_raw,
    conv_x,
    conv_b,
    conv_c,
    a_rate,
    dt_bias,
    skip_d,
    norm_gain,
    out_weight,
):
    sizes = tuple(lax.axis_size(name) for name in ("section", "seq", "head"))
    whole = (x_in, b_in, c_in, z_in, dt_raw, conv_x, conv_b, conv_c)
    args = [array[0] for array in whole] + [a_rate, dt_bias, skip_d, norm_gain]
    return layer(args, out_weight[0], sizes)[None]


def solution(mesh):
    return jax.shard_map(
        per_device,
        mesh=mesh,
        in_specs=(
            P("section", "seq", "head"),
            P("section", "seq", "head"),
            P("section", "seq", "head"),
            P("section", "seq", "head"),
            P("section", "head", "seq"),
            P("section", None, "head"),
            P("section", None, "head"),
            P("section", None, "head"),
            P("section", "head"),
            P("section", "head"),
            P("section", "head"),
            P("section", "head"),
            P("section", "head", "seq"),
        ),
        out_specs=P("section", ("seq", "head"), None),
        check_vma=False,
    )
```
